32 devices in a mesh: ctx: 2 (over core), head: 4 (over y, x), doc: 4 (over z).
Axes of the slice: x: 2, y: 2, z: 4, core: 2. Of those that a mesh axis runs over, the one named last changes fastest.
Arguments:
- queries: bfloat16 [4, 256, 8192], P('doc', 'ctx', 'head'), may hold values from -360 to 360
- keys: bfloat16 [4, 8192, 1024], P('doc', 'ctx', 'head'), may hold values from -6 to 6
- values: bfloat16 [4, 8192, 1024], P('doc', 'ctx', 'head'), may hold values from -6 to 6
- pattern: int32 [4, 2, 16], P('doc'), may hold values from 0 to 63, as said below
Outputs:
- attended: bfloat16 [4, 256, 8192], P('doc', 'ctx', 'head')
- gram: float32 [8192, 8192], P(('head', 'ctx'), 'doc')
The draws below stay inside these ranges and needn't reach their ends.
Inputs may be any that keep to these rules, and one draw needn't show every extreme that they name: Each row pattern[d, b, :] lists 16 different block numbers; no context shard (blocks s * 32 to (s + 1) * 32 - 1) holds more than 12 of one row's blocks, and in every draw some row has exactly 12 of its blocks in one shard.
All inputs are finite; a program needn't handle non-finite values.
Results may differ from the reference program's by a relative error of at most 0.015.
Values may be sent and summed in bfloat16 or wider, within the bound.
A program may use at most 128 MiB of HBM per device.

```python
import jax
import jax.numpy as jnp
from jax import lax

D = 8192
QUERY_HEADS = 64
KEY_VALUE_HEADS = 8
HEAD_SIZE = 128
BLOCK_TOKENS = 128
TOPK_DEV = 8
NKB_DEV = 32
DOCUMENT_COUNT = 4
QB = 2
QLEN = 256
CACHE_BLOCKS = 64
CONTEXT_LENGTH = 8192
SELECTED_BLOCKS = 16
CAP = 12
N_CTX = 2


def draw_queries(key, part):
    base = jax.random.truncated_normal(key, -6.0, 6.0, (DOCUMENT_COUNT, QLEN, D), jnp.float32)
    return base.astype(jnp.bfloat16)


def draw_pattern(key, part):
    rows = DOCUMENT_COUNT * QB
    owners = N_CTX
    half = owners // 2
    pair_sum = 2 * TOPK_DEV
    first_key, owner_key, local_key, order_key, force_key = jax.random.split(jax.random.fold_in(key, 11), 5)
    first = jax.random.randint(first_key, (rows, half), pair_sum - CAP, CAP + 1)
    forced_row = jax.random.randint(force_key, (), 0, rows)
    forced = (jnp.arange(rows)[:, None] == forced_row) & (jnp.arange(half)[None, :] == 0)
    first = jnp.where(forced, CAP, first)
    paired = jnp.concatenate([first, pair_sum - first], axis=1)
    owner_order = jax.vmap(lambda k: jax.random.permutation(k, owners))(jax.random.split(owner_key, rows))
    counts = jnp.take_along_axis(paired, owner_order, axis=1)
    local = jax.vmap(lambda k: jax.random.permutation(k, NKB_DEV)[:CAP])(jax.random.split(local_key, rows * owners))
    local = local.reshape(rows, owners, CAP)
    slot = jnp.arange(CAP)[None, None, :]
    valid = (slot < counts[:, :, None]).reshape(rows, owners * CAP).astype(jnp.int32)
    blocks = (jnp.arange(owners)[None, :, None] * NKB_DEV + local).reshape(rows, owners * CAP)
    shuffle = jax.vmap(lambda k: jax.random.permutation(k, owners * CAP))(jax.random.split(order_key, rows))
    score = (1 - valid) * (owners * CAP) + shuffle
    order = jnp.argsort(score, axis=1)[:, :SELECTED_BLOCKS]
    return jnp.take_along_axis(blocks, order, axis=1).reshape(DOCUMENT_COUNT, QB, SELECTED_BLOCKS).astype(jnp.int32)


def level_of(key, extent, shards, smallest, largest):
    level = 1.0
    for axis_at, shards_of in shards:
        steps = jax.random.uniform(jax.random.fold_in(jax.random.fold_in(key, 6), axis_at), (shards_of,), jnp.float32, smallest / len(shards), largest / len(shards))
        level = level * jnp.repeat(jnp.exp(steps), extent[axis_at] // shards_of).reshape((-1,) + (1,) * (len(extent) - 1 - axis_at))
    return level


def noise(key, dims, scale, bound, pieces=(), dtype=jnp.bfloat16):
    drawn = jax.random.normal(key, dims, jnp.float32) * scale
    if len(pieces) > 0:
        drawn = level_of(key, dims, pieces, -0.22, 0.18) * drawn
    return jnp.clip(drawn, min=-bound, max=bound).astype(dtype)


def setup_inputs(seed: int = 0) -> dict:
    key_of = jax.random.split(jax.random.key(seed), 5)
    queries = draw_queries(jax.random.fold_in(key_of[4], 71), 0)
    keys = noise(key_of[1], (DOCUMENT_COUNT, CONTEXT_LENGTH, KEY_VALUE_HEADS * HEAD_SIZE), 1.0, 6.0, ((0, 4), (1, 2), (2, 4)))
    values = noise(key_of[2], (DOCUMENT_COUNT, CONTEXT_LENGTH, KEY_VALUE_HEADS * HEAD_SIZE), 1.0, 6.0, ((0, 4), (1, 2), (2, 4)))
    pattern = draw_pattern(jax.random.fold_in(key_of[4], 71), 0)
    return dict(queries=queries, keys=keys, values=values, pattern=pattern)


def attend_tile(query, keys, values):
    scores = jnp.einsum("qkgd,skd->kgqs", query, keys) * (HEAD_SIZE ** -0.5)
    top = jnp.max(scores, axis=-1, keepdims=True)
    weights = jnp.exp(scores - top)
    total = jnp.sum(weights, axis=-1)
    rounded = lax.optimization_barrier(weights.astype(jnp.bfloat16))
    mixed = jnp.einsum("kgqs,skd->kgqd", rounded.astype(jnp.float32), values)
    return mixed / total[..., None]


def reference(queries, keys, values, pattern):
    every_block_list = QB * DOCUMENT_COUNT
    query_block_list = queries.reshape(every_block_list, BLOCK_TOKENS, KEY_VALUE_HEADS, QUERY_HEADS // KEY_VALUE_HEADS, HEAD_SIZE).astype(jnp.float32)
    doc_index = (jnp.arange(every_block_list) // QB).astype(jnp.int32)
    chosen = pattern.reshape(every_block_list, SELECTED_BLOCKS).astype(jnp.int32)

    def one_block(items):
        query, document_number, picked_blocks = items
        document_keys = keys[document_number].reshape(CACHE_BLOCKS, BLOCK_TOKENS, KEY_VALUE_HEADS * HEAD_SIZE)
        document_values = values[document_number].reshape(CACHE_BLOCKS, BLOCK_TOKENS, KEY_VALUE_HEADS * HEAD_SIZE)
        key_row_list = document_keys[picked_blocks].reshape(SELECTED_BLOCKS * BLOCK_TOKENS, KEY_VALUE_HEADS, HEAD_SIZE).astype(jnp.float32)
        value_row_list = document_values[picked_blocks].reshape(SELECTED_BLOCKS * BLOCK_TOKENS, KEY_VALUE_HEADS, HEAD_SIZE).astype(jnp.float32)
        mixed = attend_tile(query, key_row_list, value_row_list)
        return jnp.transpose(mixed, (2, 0, 1, 3)).reshape(BLOCK_TOKENS, D).astype(jnp.bfloat16)

    attended = lax.map(one_block, (query_block_list, doc_index, chosen)).reshape(DOCUMENT_COUNT, QLEN, D)
    flat = attended.reshape(DOCUMENT_COUNT * QLEN, D)
    gram = jnp.dot(flat.T, flat, preferred_element_type=jnp.float32)
    return attended, gram
```

```python
import functools
import math

import jax
import jax.numpy as jnp
from jax import lax
from jax.experimental import pallas as pl
from jax.experimental.pallas import tpu as pltpu
from jax.sharding import PartitionSpec as P

HEAD_SIZE = 128
BLOCK_TOKENS = 128
GROUP = 8
WIDE = 2 * HEAD_SIZE
LAG = 3
LEAD = 2
EDGE_LEAD = 0
DIRECT = 8
CAP = 12
MESH = pl.DeviceIdType.MESH


def pack_kernel(pat, k_ref, v_ref, own_ref, give_ref, sem):
    c = lax.axis_index("ctx")
    entries = pat.shape[2]
    shard_blocks = k_ref.shape[0] // BLOCK_TOKENS

    def each(action, otherwise):
        for n, (row, out_ref) in enumerate(((1 - c, give_ref), (c, own_ref))):
            for p in range(entries):
                at = pat[0, row, p] - c * shard_blocks
                mine = jnp.logical_and(at >= 0, at < shard_blocks)
                here = pl.ds(p * BLOCK_TOKENS, BLOCK_TOKENS)

                @pl.when(mine)
                def _():
                    there = pl.ds(pl.multiple_of(at * BLOCK_TOKENS, BLOCK_TOKENS), BLOCK_TOKENS)
                    for m, ref in enumerate((k_ref, v_ref)):
                        action(pltpu.make_async_copy(ref.at[there, :], out_ref.at[m, here, :], sem.at[n, m, p]))

                if otherwise:
                    @pl.when(jnp.logical_not(mine))
                    def _():
                        zero = jnp.zeros((BLOCK_TOKENS, k_ref.shape[1]), out_ref.dtype)
                        out_ref[0, here, :] = zero
                        out_ref[1, here, :] = zero

    each(lambda copy: copy.start(), True)
    each(lambda copy: copy.wait(), False)


def plain_kernel(q_any, own_any, give_any, att_ref, q_ref, own, recv, kv, in_sem, kv_send, kv_recv):
    peer = 1 - lax.axis_index("ctx")
    take_q = pltpu.make_async_copy(q_any, q_ref, in_sem.at[0])
    take_own = pltpu.make_async_copy(own_any, own, in_sem.at[0])
    take_own.start()
    take_q.start()
    barrier = pltpu.get_barrier_semaphore()
    pl.semaphore_signal(barrier, inc=1, device_id={"ctx": peer}, device_id_type=MESH)
    pl.semaphore_wait(barrier, 1)
    swaps = [remote(give_any.at[n], recv.at[n], kv_send.at[n], kv_recv.at[n], {"ctx": peer}) for n in range(2)]
    for swap in swaps:
        swap.start()
    take_q.wait()
    take_own.wait()
    for n, swap in enumerate(swaps):
        swap.wait()
        kv[n] = own[n] + recv[n]

    def plain(t, carry):
        at = pl.multiple_of(t * WIDE, WIDE)
        lane = pl.ds(pl.multiple_of((t * 2 // GROUP) * HEAD_SIZE, HEAD_SIZE), HEAD_SIZE)
        att_ref[:, pl.ds(at, WIDE)] = two_heads(q_ref[:, pl.ds(at, WIDE)], kv[0, :, lane], kv[1, :, lane])
        return carry

    lax.fori_loop(0, q_ref.shape[1] // WIDE, plain, 0)


def remote(src, dst, send, arrive, where):
    return pltpu.make_async_remote_copy(src_ref=src, dst_ref=dst, send_sem=send, recv_sem=arrive,
                                        device_id=where, device_id_type=MESH)


def two_heads(pair, keys, values):
    tokens = pair.shape[0]
    factor = HEAD_SIZE ** (-0.5) * math.log2(math.e)
    q2 = jnp.concatenate([pair[:, :HEAD_SIZE], pair[:, HEAD_SIZE:]], axis=0)
    scores = lax.dot_general(q2, keys, (((1,), (1,)), ((), ())), preferred_element_type=jnp.float32)
    top = jnp.max(scores, axis=-1, keepdims=True)
    weights = jnp.exp2((scores - top) * factor)
    total = jnp.sum(weights, axis=-1, keepdims=True)
    mixed = jnp.dot(weights.astype(jnp.bfloat16), values, preferred_element_type=jnp.float32)
    out = (mixed / total).astype(jnp.bfloat16)
    return jnp.concatenate([out[:tokens], out[tokens:]], axis=1)


def main_kernel(docs, pat, q_any, k_any, v_any, acc, buf, rows_peer, cols_peer,
                lists, q_ref, give, kv, in_sem, kv_sem, kv_send, kv_recv,
                z_up, z_down, z_recv, x_send, x_more, x_recv, r_send, r_recv, p_send, p_recv, *pieces):
    c = lax.axis_index("ctx")
    h = lax.axis_index("head")
    d = lax.axis_index("doc")
    peer = 1 - c
    tokens, width = q_ref.shape
    chunks = width // WIDE
    half = chunks // 2
    groups = kv.shape[0]
    shard = [pieces[2 * g:2 * g + 2] for g in range(groups)]
    recv = [pieces[2 * (groups + g):2 * (groups + g) + 2] for g in range(groups)]
    shard_blocks = k_any.shape[0]
    entries = pat.shape[2]
    x_next = h + 1 - 2 * (h % 2)
    y_next = (h + 2) % 4

    take_q = pltpu.make_async_copy(q_any, q_ref, in_sem.at[0])

    def take(g, m):
        lane = pl.ds(g * HEAD_SIZE, HEAD_SIZE)
        return pltpu.make_async_copy((k_any, v_any)[m].at[:, :, lane], shard[g][m], kv_sem.at[g, m])

    for g in range(groups):
        for m in range(2):
            take(g, m).start()
        if g == 0:
            take_q.start()

    barrier = pltpu.get_barrier_semaphore()

    def greet(where):
        pl.semaphore_signal(barrier, inc=1, device_id=where, device_id_type=MESH)

    greet({"ctx": peer})
    greet({"head": x_next})
    greet({"head": y_next})

    @pl.when(d > 0)
    def _():
        greet({"doc": d - 1})

    @pl.when(d < docs - 1)
    def _():
        greet({"doc": d + 1})

    for n, row in enumerate((peer, c)):
        count = jnp.int32(0)
        picked = [jnp.int32(0)] * CAP
        for p in range(entries):
            at = pat[0, row, p] - c * shard_blocks
            mine = jnp.logical_and(at >= 0, at < shard_blocks)
            hit = jnp.where(mine, count, -1)
            for s in range(min(p + 1, CAP)):
                picked[s] = jnp.where(hit == s, at, picked[s])
            count = count + jnp.where(mine, 1, 0)
        for s in range(CAP):
            lists[n, s] = picked[s]
        lists[n, CAP] = count

    def block(g, m, n, s):
        return shard[g][m][lists[n, s]]

    def swap(g, m):
        return remote(give.at[g, m], recv[g][m], kv_send.at[g, m], kv_recv.at[g, m], {"ctx": peer})

    def place_of(s):
        return pl.ds(s * BLOCK_TOKENS, BLOCK_TOKENS)

    ends = jnp.where(d > 0, 1, 0) + jnp.where(d < docs - 1, 1, 0)
    for g in range(groups):
        for m in range(2):
            take(g, m).wait()
            for s in range(CAP):
                give[g, m, s] = block(g, m, 0, s)
            if g == 0 and m == 0:
                pl.semaphore_wait(barrier, 3 + ends)
            swap(g, m).start()
    for g in range(groups):
        for m in range(2):
            for s in range(CAP):
                kv[g, m, place_of(s), :] = block(g, m, 1, s)
    take_q.wait()

    def merge(g):
        own = lists[1, CAP]
        for m in range(2):
            swap(g, m).wait_recv()
            for s in range(entries - CAP, entries):
                came = recv[g][m][jnp.clip(s - own, 0, CAP - 1)]
                if s < CAP:
                    came = jnp.where(jnp.full(came.shape, own) > s, kv[g, m, place_of(s), :], came)
                kv[g, m, place_of(s), :] = came

    total_events = docs * chunks
    far = jnp.maximum(d, docs - 1 - d)
    rx = (h % 2 + d % 2) % 2
    ry = (h // 2 + d // 2) % 2
    source = jnp.where(h == d, 0, 1)

    def up(i, k):
        return remote(buf.at[0, i, k], buf.at[0, i, k], z_up.at[i, k], z_recv.at[i, k], {"doc": d + 1})

    def down(i, k):
        return remote(buf.at[0, i, k], buf.at[0, i, k], z_down.at[i, k], z_recv.at[i, k], {"doc": d - 1})

    def row_copy(i, k):
        return remote(buf.at[0, i, k], rows_peer.at[i, k % half], r_send.at[i, k], r_recv.at[i, k], {"ctx": peer})

    def col_copy(i, k):
        return remote(buf.at[source, i, k], cols_peer.at[i, k], p_send.at[i, k], p_recv.at[i, k], {"ctx": peer})

    def plane_copy(i, k, sem, head):
        return remote(buf.at[source, i, k], buf.at[1, i, k], sem.at[i, k], x_recv.at[i, k], {"head": head})

    def place(k):
        even = k % 2 == 0
        return (jnp.where(even, rx, ry), jnp.where(even, ry, rx),
                jnp.where(even, x_next, y_next), jnp.where(even, y_next, x_next))

    def is_direct(s, k):
        return jnp.logical_and(s == far, k >= chunks - DIRECT)

    def item(side, s):
        i = d - s if side == 0 else d + s
        there = (i >= 0) if side == 0 else jnp.logical_and(i < docs, s > 0)
        return i, there

    def z_part(e):
        s, k = e // chunks, e % chunks
        for side in range(2):
            i, there = item(side, s)

            @pl.when(there)
            def _():
                @pl.when(s > 0)
                def _():
                    up(i, k).wait_recv()

                @pl.when(jnp.logical_and(i <= d, d < docs - 1))
                def _():
                    up(i, k).start()

                @pl.when(jnp.logical_and(i >= d, d > 0))
                def _():
                    down(i, k).start()

                @pl.when(k // half != c)
                def _():
                    row_copy(i, k).start()

    def z_ahead(e):
        def bound(e):
            return jnp.clip(e + 1 + lead, chunks, total_events)

        def one(n, carry):
            z_part(n)
            return carry

        lax.fori_loop(bound(e - 1), bound(e), one, 0)

    edge = jnp.logical_or(d == 0, d == docs - 1)
    lead = jnp.where(edge, EDGE_LEAD, LEAD)
    settle = jnp.where(edge, total_events, total_events + LAG)

    def lag(e):
        return jnp.clip(settle - e, 1, LAG)

    def x_part(e):
        for parity in range(2):
            a, b, first, second = place(parity)
            hop = a + b * (3 - 2 * a)

            def one(at, carry):
                s, k = at // chunks, at % chunks
                direct = is_direct(s, k)
                for side in range(2):
                    i, there = item(side, s)

                    @pl.when(there)
                    def _():
                        @pl.when(hop == 0)
                        def _():
                            plane_copy(i, k, x_send, first).start()

                            @pl.when(direct)
                            def _():
                                plane_copy(i, k, x_more, second).start()

                        @pl.when(hop > 0)
                        def _():
                            plane_copy(i, k, x_send, first).wait_recv()

                            @pl.when(hop == 1)
                            def _():
                                plane_copy(i, k, x_send, second).start()

                            @pl.when(jnp.logical_and(hop == 2, jnp.logical_not(direct)))
                            def _():
                                plane_copy(i, k, x_send, first).start()

                        col_copy(i, k).start()

                return carry

            def bound(e):
                return jnp.clip(e + 1 - lag(e) * hop, 0, total_events)

            def half_of(n):
                return (n + 1 - parity) // 2

            lax.fori_loop(half_of(bound(e - 1)), half_of(bound(e)), lambda n, carry: one(2 * n + parity, carry), 0)

    def document(n):
        middle = jnp.where(n == 0, d, jnp.where(n == 1, d - 1, d + 1))
        return jnp.where(d == 0, n, jnp.where(d == docs - 1, d - n, middle))

    def arrived(i):
        def one(k, carry):
            col_copy(i, k).wait_recv()

            @pl.when(k // half == c)
            def _():
                row_copy(i, k).wait_recv()

            return carry

        lax.fori_loop(0, chunks, one, 0)

    def piece(n, carry):
        i, r = document(n // half), n % half

        @pl.when(r == 0)
        def _():
            arrived(i)

        @pl.when(n < half)
        def _():
            add_piece(c, i, r, source, None, acc, buf, rows_peer, cols_peer)

        @pl.when(n >= half)
        def _():
            add_piece(c, i, r, source, acc, acc, buf, rows_peer, cols_peer)

        return carry

    def gram_part(e):
        def done(e):
            first = jnp.clip(e + 1 - chunks - 3 * LAG, 0, half)
            second = jnp.clip(e + 1 - 2 * chunks - 3 * LAG, 0, half)
            third = jnp.where(edge, 2 * jnp.clip(e + 2 - total_events, 0, half // 2),
                              jnp.clip(e + 1 - 2 * chunks - half - 3 * LAG, 0, half))
            return first + second + third

        lax.fori_loop(done(e - 1), done(e), piece, 0)

    def opening(e, carry):
        g = e * 2 // GROUP

        for n in range(groups):
            @pl.when(e == n * GROUP // 2)
            def _():
                merge(n)

        buf[0, d, e] = two_heads(q_ref[:, pl.ds(pl.multiple_of(e * WIDE, WIDE), WIDE)], kv[g, 0], kv[g, 1])
        z_part(e)
        z_ahead(e)
        x_part(e)
        return carry

    def event(e, carry):
        z_ahead(e)
        x_part(e)
        gram_part(e)
        return carry

    lax.fori_loop(0, chunks, opening, 0)
    lax.fori_loop(chunks, total_events + LAG, event, 0)

    for g in range(groups):
        for m in range(2):
            swap(g, m).wait_send()

    def finish(n, carry):
        i, k = n // chunks, n % chunks
        a, b, first, second = place(k)
        hop = a + b * (3 - 2 * a)
        direct = is_direct(jnp.maximum(i - d, d - i), k)

        @pl.when(jnp.logical_and(i <= d, d < docs - 1))
        def _():
            up(i, k).wait_send()

        @pl.when(jnp.logical_and(i >= d, d > 0))
        def _():
            down(i, k).wait_send()

        @pl.when(k // half != c)
        def _():
            row_copy(i, k).wait_send()

        col_copy(i, k).wait_send()

        @pl.when(jnp.logical_or(hop < 2, jnp.logical_and(hop == 2, jnp.logical_not(direct))))
        def _():
            plane_copy(i, k, x_send, first).wait_send()

        @pl.when(jnp.logical_and(hop == 0, direct))
        def _():
            plane_copy(i, k, x_more, second).wait_send()

        return carry

    lax.fori_loop(0, total_events, finish, 0)
    arrived(document(docs - 1) if docs == 2 else jnp.where(d < docs // 2, docs - 1, 0))


def add_piece(c, i, r, source, before, after, buf, rows_peer, cols_peer):
    chunks = cols_peer.shape[1]
    here = pl.ds(pl.multiple_of(r * WIDE, WIDE), WIDE)
    left = jnp.concatenate([buf[0, i, c * (chunks // 2) + r], rows_peer[i, r]], axis=0)
    for k in range(chunks):
        right = jnp.concatenate([buf[source, i, k], cols_peer[i, k]], axis=0)
        lane = pl.ds(k * WIDE, WIDE)
        product = lax.dot_general(left, right, (((0,), (0,)), ((), ())), preferred_element_type=jnp.float32)
        after[here, lane] = product if before is None else before[here, lane] + product


def last_kernel(docs, acc, buf, rows_peer, cols_peer, att_ref, gram_ref, stage, att_sem, gram_sem):
    c = lax.axis_index("ctx")
    h = lax.axis_index("head")
    d = lax.axis_index("doc")
    chunks = cols_peer.shape[1]
    source = jnp.where(h == d, 0, 1)
    i = jnp.where(d < docs // 2, docs - 1, 0)

    def give(r):
        here = pl.ds(r * WIDE, WIDE)
        return pltpu.make_async_copy(stage.at[here, :], gram_ref.at[here, :], gram_sem.at[r])

    def put(k):
        return pltpu.make_async_copy(buf.at[0, d, k], att_ref.at[:, pl.ds(k * WIDE, WIDE)], att_sem.at[k])

    for k in range(chunks):
        put(k).start()
    for r in range(chunks // 2):
        add_piece(c, i, r, source, acc, stage, buf, rows_peer, cols_peer)
        give(r).start()
    for k in range(chunks):
        put(k).wait()
    for r in range(chunks // 2):
        give(r).wait()


def plain(queries, keys, values, pattern):
    tokens, width = queries.shape
    wide = keys.shape[1]
    entries = pattern.shape[2]
    vmem = pl.BlockSpec(memory_space=pltpu.VMEM)
    smem = pl.BlockSpec(memory_space=pltpu.SMEM)
    hbm = pl.BlockSpec(memory_space=pl.ANY)
    pack = (2, entries * BLOCK_TOKENS, wide)
    own, give = pl.pallas_call(
        pack_kernel,
        out_shape=[jax.ShapeDtypeStruct(pack, jnp.bfloat16)] * 2,
        in_specs=[smem, hbm, hbm],
        out_specs=[vmem] * 2,
        scratch_shapes=[pltpu.SemaphoreType.DMA((2, 2, entries))],
    )(pattern, keys, values)
    scratch = [pltpu.VMEM((tokens, width), jnp.bfloat16)] + [pltpu.VMEM(pack, jnp.bfloat16)] * 3
    return pl.pallas_call(
        plain_kernel,
        out_shape=jax.ShapeDtypeStruct((tokens, width), jnp.bfloat16),
        in_specs=[hbm] * 3,
        out_specs=vmem,
        scratch_shapes=scratch + [pltpu.SemaphoreType.DMA((2,))] * 3,
        compiler_params=pltpu.CompilerParams(collective_id=0, has_side_effects=True),
    )(queries, own, give)


def fused(queries, keys, values, pattern, docs):
    tokens, width = queries.shape
    shard_rows, wide = keys.shape
    groups = wide // HEAD_SIZE
    entries = pattern.shape[2]
    chunks = width // WIDE
    bf16, f32 = jnp.bfloat16, jnp.float32
    vmem = pl.BlockSpec(memory_space=pltpu.VMEM)
    hbm = pl.BlockSpec(memory_space=pl.ANY)
    held = [
        pltpu.VMEM((width // 2, width), f32),
        pltpu.VMEM((2, docs, chunks, tokens, WIDE), bf16),
        pltpu.VMEM((docs, chunks // 2, tokens, WIDE), bf16),
        pltpu.VMEM((docs, chunks, tokens, WIDE), bf16),
    ]
    blocks = (shard_rows // BLOCK_TOKENS, BLOCK_TOKENS)
    made = pl.pallas_call(
        functools.partial(main_kernel, docs),
        out_shape=held,
        in_specs=[pl.BlockSpec(memory_space=pltpu.SMEM)] + [hbm] * 3,
        out_specs=[vmem] * 4,
        scratch_shapes=[
            pltpu.SMEM((2, CAP + 1), jnp.int32),
            pltpu.VMEM((tokens, width), bf16),
            pltpu.VMEM((groups, 2, CAP, BLOCK_TOKENS, HEAD_SIZE), bf16),
            pltpu.VMEM((groups, 2, entries * BLOCK_TOKENS, HEAD_SIZE), bf16),
            pltpu.SemaphoreType.DMA((1,)),
        ] + [pltpu.SemaphoreType.DMA((groups, 2))] * 3 + [pltpu.SemaphoreType.DMA((docs, chunks))] * 10
        + [pltpu.VMEM(blocks + (HEAD_SIZE,), bf16)] * (2 * groups)
        + [pltpu.VMEM((CAP, BLOCK_TOKENS, HEAD_SIZE), bf16)] * (2 * groups),
        compiler_params=pltpu.CompilerParams(
            collective_id=0, has_side_effects=True, vmem_limit_bytes=51314688),
    )(pattern, queries, keys.reshape(blocks + (wide,)), values.reshape(blocks + (wide,)))
    return pl.pallas_call(
        functools.partial(last_kernel, docs),
        out_shape=[
            jax.ShapeDtypeStruct((tokens, width), bf16),
            jax.ShapeDtypeStruct((width // 2, width), f32),
        ],
        in_specs=[vmem] * 4,
        out_specs=[hbm] * 2,
        scratch_shapes=[
            pltpu.VMEM((width // 2, width), f32),
            pltpu.SemaphoreType.DMA((chunks,)),
            pltpu.SemaphoreType.DMA((chunks // 2,)),
        ],
        compiler_params=pltpu.CompilerParams(vmem_limit_bytes=32 << 20),
    )(*made)


def per_device(queries, keys, values, pattern):
    ctx_count = lax.axis_size("ctx")
    head_count = lax.axis_size("head")
    doc_count = lax.axis_size("doc")
    owner = lax.axis_index("ctx")
    tok_rows = queries.shape[1]
    width = queries.shape[2]
    direct = head_count == 4 and doc_count == 4
    contract = (((0,), (0,)), ((), ()))
    if direct:
        attended, product = fused(queries[0], keys[0], values[0], pattern, doc_count)
        return (attended[None], product)
    attended = plain(queries[0], keys[0], values[0], pattern)
    sub = width // ctx_count
    model_width = width * head_count
    span = lax.all_gather(attended, "ctx", axis=0, tiled=True)
    mine_cols = lax.dynamic_slice_in_dim(span, owner * sub, sub, 1)
    full_doc = lax.all_gather(span, "head", axis=1, tiled=True)
    slice_width = model_width // doc_count
    split_cols = full_doc.reshape(tok_rows * ctx_count, doc_count, slice_width)
    column_set = lax.all_to_all(split_cols, "doc", split_axis=1, concat_axis=0, tiled=True).reshape(
        doc_count * tok_rows * ctx_count, slice_width)
    product = lax.dot_general(
        lax.all_gather(mine_cols, "doc", axis=0, tiled=True), column_set, contract,
        preferred_element_type=jnp.float32)
    return (attended[None], product)


def solution(mesh):
    placed = (
        P("doc", "ctx", "head"),
        P("doc", "ctx", "head"),
        P("doc", "ctx", "head"),
        P("doc", None, None),
    )
    return jax.shard_map(
        per_device,
        mesh=mesh,
        in_specs=placed,
        out_specs=(P("doc", "ctx", "head"), P(("head", "ctx"), "doc")),
        check_vma=False,
    )
```

```python
import functools
import math

import jax
import jax.numpy as jnp
from jax import lax
from jax.experimental import pallas as pl
from jax.experimental.pallas import tpu as pltpu
from jax.sharding import PartitionSpec as P

HEAD_SIZE = 128
BLOCK_TOKENS = 128
GROUP = 8
WIDE = 2 * HEAD_SIZE
LAG = 3
LEAD = 2
EDGE_LEAD = 0
DIRECT = 8
CAP = 12
SPENT = 11
PARTS = 1
MESH = pl.DeviceIdType.MESH


def pack_kernel(pat, k_ref, v_ref, own_ref, give_ref, sem):
    c = lax.axis_index("ctx")
    entries = pat.shape[2]
    shard_blocks = k_ref.shape[0] // BLOCK_TOKENS

    def each(action, otherwise):
        for n, (row, out_ref) in enumerate(((1 - c, give_ref), (c, own_ref))):
            for p in range(entries):
                at = pat[0, row, p] - c * shard_blocks
                mine = jnp.logical_and(at >= 0, at < shard_blocks)
                here = pl.ds(p * BLOCK_TOKENS, BLOCK_TOKENS)

                @pl.when(mine)
                def _():
                    there = pl.ds(pl.multiple_of(at * BLOCK_TOKENS, BLOCK_TOKENS), BLOCK_TOKENS)
                    for m, ref in enumerate((k_ref, v_ref)):
                        action(pltpu.make_async_copy(ref.at[there, :], out_ref.at[m, here, :], sem.at[n, m, p]))

                if otherwise:
                    @pl.when(jnp.logical_not(mine))
                    def _():
                        zero = jnp.zeros((BLOCK_TOKENS, k_ref.shape[1]), out_ref.dtype)
                        out_ref[0, here, :] = zero
                        out_ref[1, here, :] = zero

    each(lambda copy: copy.start(), True)
    each(lambda copy: copy.wait(), False)


def plain_kernel(q_any, own_any, give_any, att_ref, q_ref, own, recv, kv, in_sem, kv_send, kv_recv):
    peer = 1 - lax.axis_index("ctx")
    take_q = pltpu.make_async_copy(q_any, q_ref, in_sem.at[0])
    take_own = pltpu.make_async_copy(own_any, own, in_sem.at[0])
    take_own.start()
    take_q.start()
    barrier = pltpu.get_barrier_semaphore()
    pl.semaphore_signal(barrier, inc=1, device_id={"ctx": peer}, device_id_type=MESH)
    pl.semaphore_wait(barrier, 1)
    swaps = [remote(give_any.at[n], recv.at[n], kv_send.at[n], kv_recv.at[n], {"ctx": peer}) for n in range(2)]
    for swap in swaps:
        swap.start()
    take_q.wait()
    take_own.wait()
    for n, swap in enumerate(swaps):
        swap.wait()
        kv[n] = own[n] + recv[n]

    def plain(t, carry):
        at = pl.multiple_of(t * WIDE, WIDE)
        lane = pl.ds(pl.multiple_of((t * 2 // GROUP) * HEAD_SIZE, HEAD_SIZE), HEAD_SIZE)
        att_ref[:, pl.ds(at, WIDE)] = two_heads(q_ref[:, pl.ds(at, WIDE)], kv[0, :, lane], kv[1, :, lane])
        return carry

    lax.fori_loop(0, q_ref.shape[1] // WIDE, plain, 0)


def remote(src, dst, send, arrive, where):
    return pltpu.make_async_remote_copy(src_ref=src, dst_ref=dst, send_sem=send, recv_sem=arrive,
                                        device_id=where, device_id_type=MESH)


def two_heads(pair, keys, values):
    tokens = pair.shape[0]
    factor = HEAD_SIZE ** (-0.5) * math.log2(math.e)
    q2 = jnp.concatenate([pair[:, :HEAD_SIZE], pair[:, HEAD_SIZE:]], axis=0)
    scores = lax.dot_general(q2, keys, (((1,), (1,)), ((), ())), preferred_element_type=jnp.float32)
    top = jnp.max(scores, axis=-1, keepdims=True)
    weights = jnp.exp2((scores - top) * factor)
    total = jnp.sum(weights, axis=-1, keepdims=True)
    mixed = jnp.dot(weights.astype(jnp.bfloat16), values, preferred_element_type=jnp.float32)
    out = (mixed / total).astype(jnp.bfloat16)
    return jnp.concatenate([out[:tokens], out[tokens:]], axis=1)


def main_kernel(docs, pat, q_any, k_any, v_any, acc, buf, rows_peer, cols_peer,
                lists, q_ref, give, kv, in_sem, kv_sem, kv_send, kv_recv,
                z_up, z_down, z_recv, x_send, x_more, x_recv, r_send, r_recv, p_send, p_recv, *pieces):
    c = lax.axis_index("ctx")
    h = lax.axis_index("head")
    d = lax.axis_index("doc")
    peer = 1 - c
    tokens, width = q_ref.shape
    chunks = width // WIDE
    half = chunks // 2
    groups = kv.shape[0]
    shard = [pieces[2 * g:2 * g + 2] for g in range(groups)]
    recv = [pieces[2 * (groups + g):2 * (groups + g) + 2] for g in range(groups)]
    shard_blocks = k_any.shape[0]
    entries = pat.shape[2]
    x_next = h + 1 - 2 * (h % 2)
    y_next = (h + 2) % 4

    take_q = pltpu.make_async_copy(q_any, q_ref, in_sem.at[0])

    def take(g, m):
        lane = pl.ds(g * HEAD_SIZE, HEAD_SIZE)
        return pltpu.make_async_copy((k_any, v_any)[m].at[:, :, lane], shard[g][m], kv_sem.at[g, m])

    for g in range(groups):
        for m in range(2):
            take(g, m).start()
        if g == 0:
            take_q.start()

    barrier = pltpu.get_barrier_semaphore()

    def greet(where):
        pl.semaphore_signal(barrier, inc=1, device_id=where, device_id_type=MESH)

    greet({"ctx": peer})
    greet({"head": x_next})
    greet({"head": y_next})

    @pl.when(d > 0)
    def _():
        greet({"doc": d - 1})

    @pl.when(d < docs - 1)
    def _():
        greet({"doc": d + 1})

    for n, row in enumerate((peer, c)):
        count = jnp.int32(0)
        picked = [jnp.int32(0)] * CAP
        for p in range(entries):
            at = pat[0, row, p] - c * shard_blocks
            mine = jnp.logical_and(at >= 0, at < shard_blocks)
            hit = jnp.where(mine, count, -1)
            for s in range(min(p + 1, CAP)):
                picked[s] = jnp.where(hit == s, at, picked[s])
            count = count + jnp.where(mine, 1, 0)
        for s in range(CAP):
            lists[n, s] = picked[s]
        lists[n, CAP] = count

    def block(g, m, n, s):
        return shard[g][m][lists[n, s]]

    def swap(g, m):
        return remote(give.at[g, m], recv[g][m], kv_send.at[g, m], kv_recv.at[g, m], {"ctx": peer})

    def place_of(s):
        return pl.ds(s * BLOCK_TOKENS, BLOCK_TOKENS)

    ends = jnp.where(d > 0, 1, 0) + jnp.where(d < docs - 1, 1, 0)
    for g in range(groups):
        for m in range(2):
            take(g, m).wait()
            for s in range(CAP):
                give[g, m, s] = block(g, m, 0, s)
            if g == 0 and m == 0:
                pl.semaphore_wait(barrier, 3 + ends)
            swap(g, m).start()
    for g in range(groups):
        for m in range(2):
            for s in range(CAP):
                kv[g, m, place_of(s), :] = block(g, m, 1, s)
    take_q.wait()

    def merge(g):
        own = lists[1, CAP]
        for m in range(2):
            swap(g, m).wait_recv()
            for s in range(entries - CAP, entries):
                came = recv[g][m][jnp.clip(s - own, 0, CAP - 1)]
                if s < CAP:
                    came = jnp.where(jnp.full(came.shape, own) > s, kv[g, m, place_of(s), :], came)
                kv[g, m, place_of(s), :] = came

    total_events = docs * chunks
    far = jnp.maximum(d, docs - 1 - d)
    rx = (h % 2 + d % 2) % 2
    ry = (h // 2 + d // 2) % 2
    source = jnp.where(h == d, 0, 1)

    def part_of(p):
        return pl.ds(p * (tokens // PARTS), tokens // PARTS)

    def up(i, k, p):
        ref = buf.at[0, i, k, part_of(p)]
        return remote(ref, ref, z_up.at[i, k, p], z_recv.at[i, k, p], {"doc": d + 1})

    def down(i, k, p):
        ref = buf.at[0, i, k, part_of(p)]
        return remote(ref, ref, z_down.at[i, k, p], z_recv.at[i, k, p], {"doc": d - 1})

    def row_copy(i, k):
        return remote(buf.at[0, i, k], rows_peer.at[i, k % half], r_send.at[i, k], r_recv.at[i, k], {"ctx": peer})

    def col_copy(i, k):
        return remote(buf.at[source, i, k], cols_peer.at[i, k], p_send.at[i, k], p_recv.at[i, k], {"ctx": peer})

    def plane_copy(i, k, p, sem, head):
        return remote(buf.at[source, i, k, part_of(p)], buf.at[1, i, k, part_of(p)], sem.at[i, k, p],
                      x_recv.at[i, k, p], {"head": head})

    def place(k):
        even = k % 2 == 0
        return (jnp.where(even, rx, ry), jnp.where(even, ry, rx),
                jnp.where(even, x_next, y_next), jnp.where(even, y_next, x_next))

    def is_direct(s, k):
        return jnp.logical_and(s == far, k >= chunks - DIRECT)

    def item(side, s):
        i = d - s if side == 0 else d + s
        there = (i >= 0) if side == 0 else jnp.logical_and(i < docs, s > 0)
        return i, there

    def z_part(e):
        s, k = e // chunks, e % chunks
        for side in range(2):
            i, there = item(side, s)

            @pl.when(there)
            def _():
                for p in range(PARTS):
                    @pl.when(s > 0)
                    def _():
                        up(i, k, p).wait_recv()

                    @pl.when(jnp.logical_and(i <= d, d < docs - 1))
                    def _():
                        up(i, k, p).start()

                    @pl.when(jnp.logical_and(i >= d, d > 0))
                    def _():
                        down(i, k, p).start()

                @pl.when(k // half != c)
                def _():
                    row_copy(i, k).start()

    def z_ahead(e):
        def bound(e):
            return jnp.clip(e + 1 + lead, chunks, total_events)

        def one(n, carry):
            z_part(n)
            return carry

        lax.fori_loop(bound(e - 1), bound(e), one, 0)

    edge = jnp.logical_or(d == 0, d == docs - 1)
    lead = jnp.where(edge, EDGE_LEAD, LEAD)
    settle = jnp.where(edge, total_events, total_events + LAG)

    def lag(e):
        return jnp.clip(settle - e, 1, LAG)

    def x_part(e):
        for parity in range(2):
            a, b, first, second = place(parity)
            hop = a + b * (3 - 2 * a)

            def one(at, carry):
                s, k = at // chunks, at % chunks
                direct = is_direct(s, k)
                for side in range(2):
                    i, there = item(side, s)

                    @pl.when(there)
                    def _():
                        for p in range(PARTS):
                            @pl.when(hop == 0)
                            def _():
                                plane_copy(i, k, p, x_send, first).start()

                                @pl.when(direct)
                                def _():
                                    plane_copy(i, k, p, x_more, second).start()

                            @pl.when(hop > 0)
                            def _():
                                plane_copy(i, k, p, x_send, first).wait_recv()

                                @pl.when(hop == 1)
                                def _():
                                    plane_copy(i, k, p, x_send, second).start()

                                @pl.when(jnp.logical_and(hop == 2, jnp.logical_not(direct)))
                                def _():
                                    plane_copy(i, k, p, x_send, first).start()

                        col_copy(i, k).start()

                return carry

            def bound(e):
                return jnp.clip(e + 1 - lag(e) * hop, 0, total_events)

            def half_of(n):
                return (n + 1 - parity) // 2

            lax.fori_loop(half_of(bound(e - 1)), half_of(bound(e)), lambda n, carry: one(2 * n + parity, carry), 0)

    def document(n):
        middle = jnp.where(n == 0, d, jnp.where(n == 1, d - 1, d + 1))
        return jnp.where(d == 0, n, jnp.where(d == docs - 1, d - n, middle))

    def arrived(i):
        def one(k, carry):
            col_copy(i, k).wait_recv()

            @pl.when(k // half == c)
            def _():
                row_copy(i, k).wait_recv()

            return carry

        lax.fori_loop(0, chunks, one, 0)

    def piece(n, carry):
        i, r = document(n // half), n % half

        @pl.when(r == 0)
        def _():
            arrived(i)

        @pl.when(n < half)
        def _():
            add_piece(c, i, r, source, None, acc, buf, rows_peer, cols_peer)

        @pl.when(n >= half)
        def _():
            add_piece(c, i, r, source, acc, acc, buf, rows_peer, cols_peer)

        return carry

    def gram_part(e):
        def done(e):
            first = jnp.clip(e + 1 - chunks - 3 * LAG, 0, half)
            second = jnp.clip(e + 1 - 2 * chunks - 3 * LAG, 0, half)
            third = jnp.where(edge, 2 * jnp.clip(e + 2 - total_events, 0, half // 2),
                              jnp.clip(e + 1 - 2 * chunks - half - 3 * LAG, 0, half))
            return first + second + third

        lax.fori_loop(done(e - 1), done(e), piece, 0)

    def finish(e, carry):
        s, k = e // chunks, e % chunks
        a, b, first, second = place(k)
        hop = a + b * (3 - 2 * a)
        direct = is_direct(s, k)
        for side in range(2):
            i, there = item(side, s)

            @pl.when(there)
            def _():
                for p in range(PARTS):
                    @pl.when(jnp.logical_and(i <= d, d < docs - 1))
                    def _():
                        up(i, k, p).wait_send()

                    @pl.when(jnp.logical_and(i >= d, d > 0))
                    def _():
                        down(i, k, p).wait_send()

                    @pl.when(jnp.logical_or(hop < 2, jnp.logical_and(hop == 2, jnp.logical_not(direct))))
                    def _():
                        plane_copy(i, k, p, x_send, first).wait_send()

                    @pl.when(jnp.logical_and(hop == 0, direct))
                    def _():
                        plane_copy(i, k, p, x_more, second).wait_send()

                @pl.when(k // half != c)
                def _():
                    row_copy(i, k).wait_send()

                col_copy(i, k).wait_send()

        return carry

    def opening(e, carry):
        g = e * 2 // GROUP

        for n in range(groups):
            @pl.when(e == n * GROUP // 2)
            def _():
                merge(n)

        buf[0, d, e] = two_heads(q_ref[:, pl.ds(pl.multiple_of(e * WIDE, WIDE), WIDE)], kv[g, 0], kv[g, 1])
        z_part(e)
        z_ahead(e)
        x_part(e)
        return carry

    def event(e, carry):
        z_ahead(e)
        x_part(e)
        gram_part(e)

        @pl.when(e >= SPENT)
        def _():
            finish(e - SPENT, 0)

        return carry

    lax.fori_loop(0, chunks, opening, 0)
    for g in range(groups):
        for m in range(2):
            swap(g, m).wait_send()
    lax.fori_loop(chunks, total_events + LAG, event, 0)
    lax.fori_loop(total_events + LAG - SPENT, total_events, finish, 0)
    arrived(document(docs - 1) if docs == 2 else jnp.where(d < docs // 2, docs - 1, 0))


def add_piece(c, i, r, source, before, after, buf, rows_peer, cols_peer):
    chunks = cols_peer.shape[1]
    here = pl.ds(pl.multiple_of(r * WIDE, WIDE), WIDE)
    left = jnp.concatenate([buf[0, i, c * (chunks // 2) + r], rows_peer[i, r]], axis=0)
    for k in range(chunks):
        right = jnp.concatenate([buf[source, i, k], cols_peer[i, k]], axis=0)
        lane = pl.ds(k * WIDE, WIDE)
        product = lax.dot_general(left, right, (((0,), (0,)), ((), ())), preferred_element_type=jnp.float32)
        after[here, lane] = product if before is None else before[here, lane] + product


def last_kernel(docs, acc, buf, rows_peer, cols_peer, att_ref, gram_ref, stage, att_sem, gram_sem):
    c = lax.axis_index("ctx")
    h = lax.axis_index("head")
    d = lax.axis_index("doc")
    chunks = cols_peer.shape[1]
    source = jnp.where(h == d, 0, 1)
    i = jnp.where(d < docs // 2, docs - 1, 0)

    def give(r):
        here = pl.ds(r * WIDE, WIDE)
        return pltpu.make_async_copy(stage.at[here, :], gram_ref.at[here, :], gram_sem.at[r])

    def put(k):
        return pltpu.make_async_copy(buf.at[0, d, k], att_ref.at[:, pl.ds(k * WIDE, WIDE)], att_sem.at[k])

    for k in range(chunks):
        put(k).start()
    for r in range(chunks // 2):
        add_piece(c, i, r, source, acc, stage, buf, rows_peer, cols_peer)
        give(r).start()
    for k in range(chunks):
        put(k).wait()
    for r in range(chunks // 2):
        give(r).wait()


def plain(queries, keys, values, pattern):
    tokens, width = queries.shape
    wide = keys.shape[1]
    entries = pattern.shape[2]
    vmem = pl.BlockSpec(memory_space=pltpu.VMEM)
    smem = pl.BlockSpec(memory_space=pltpu.SMEM)
    hbm = pl.BlockSpec(memory_space=pl.ANY)
    pack = (2, entries * BLOCK_TOKENS, wide)
    own, give = pl.pallas_call(
        pack_kernel,
        out_shape=[jax.ShapeDtypeStruct(pack, jnp.bfloat16)] * 2,
        in_specs=[smem, hbm, hbm],
        out_specs=[vmem] * 2,
        scratch_shapes=[pltpu.SemaphoreType.DMA((2, 2, entries))],
    )(pattern, keys, values)
    scratch = [pltpu.VMEM((tokens, width), jnp.bfloat16)] + [pltpu.VMEM(pack, jnp.bfloat16)] * 3
    return pl.pallas_call(
        plain_kernel,
        out_shape=jax.ShapeDtypeStruct((tokens, width), jnp.bfloat16),
        in_specs=[hbm] * 3,
        out_specs=vmem,
        scratch_shapes=scratch + [pltpu.SemaphoreType.DMA((2,))] * 3,
        compiler_params=pltpu.CompilerParams(collective_id=0, has_side_effects=True),
    )(queries, own, give)


def fused(queries, keys, values, pattern, docs):
    tokens, width = queries.shape
    shard_rows, wide = keys.shape
    groups = wide // HEAD_SIZE
    entries = pattern.shape[2]
    chunks = width // WIDE
    bf16, f32 = jnp.bfloat16, jnp.float32
    vmem = pl.BlockSpec(memory_space=pltpu.VMEM)
    hbm = pl.BlockSpec(memory_space=pl.ANY)
    held = [
        pltpu.VMEM((width // 2, width), f32),
        pltpu.VMEM((2, docs, chunks, tokens, WIDE), bf16),
        pltpu.VMEM((docs, chunks // 2, tokens, WIDE), bf16),
        pltpu.VMEM((docs, chunks, tokens, WIDE), bf16),
    ]
    blocks = (shard_rows // BLOCK_TOKENS, BLOCK_TOKENS)
    made = pl.pallas_call(
        functools.partial(main_kernel, docs),
        out_shape=held,
        in_specs=[pl.BlockSpec(memory_space=pltpu.SMEM)] + [hbm] * 3,
        out_specs=[vmem] * 4,
        scratch_shapes=[
            pltpu.SMEM((2, CAP + 1), jnp.int32),
            pltpu.VMEM((tokens, width), bf16),
            pltpu.VMEM((groups, 2, CAP, BLOCK_TOKENS, HEAD_SIZE), bf16),
            pltpu.VMEM((groups, 2, entries * BLOCK_TOKENS, HEAD_SIZE), bf16),
            pltpu.SemaphoreType.DMA((1,)),
        ] + [pltpu.SemaphoreType.DMA((groups, 2))] * 3 + [pltpu.SemaphoreType.DMA((docs, chunks, PARTS))] * 6
        + [pltpu.SemaphoreType.DMA((docs, chunks))] * 4
        + [pltpu.VMEM(blocks + (HEAD_SIZE,), bf16)] * (2 * groups)
        + [pltpu.VMEM((CAP, BLOCK_TOKENS, HEAD_SIZE), bf16)] * (2 * groups),
        compiler_params=pltpu.CompilerParams(
            collective_id=0, has_side_effects=True, vmem_limit_bytes=51314688),
    )(pattern, queries, keys.reshape(blocks + (wide,)), values.reshape(blocks + (wide,)))
    return pl.pallas_call(
        functools.partial(last_kernel, docs),
        out_shape=[
            jax.ShapeDtypeStruct((tokens, width), bf16),
            jax.ShapeDtypeStruct((width // 2, width), f32),
        ],
        in_specs=[vmem] * 4,
        out_specs=[hbm] * 2,
        scratch_shapes=[
            pltpu.VMEM((width // 2, width), f32),
            pltpu.SemaphoreType.DMA((chunks,)),
            pltpu.SemaphoreType.DMA((chunks // 2,)),
        ],
        compiler_params=pltpu.CompilerParams(vmem_limit_bytes=32 << 20),
    )(*made)


def per_device(queries, keys, values, pattern):
    ctx_count = lax.axis_size("ctx")
    head_count = lax.axis_size("head")
    doc_count = lax.axis_size("doc")
    owner = lax.axis_index("ctx")
    tok_rows = queries.shape[1]
    width = queries.shape[2]
    direct = head_count == 4 and doc_count == 4
    contract = (((0,), (0,)), ((), ()))
    if direct:
        attended, product = fused(queries[0], keys[0], values[0], pattern, doc_count)
        return (attended[None], product)
    attended = plain(queries[0], keys[0], values[0], pattern)
    sub = width // ctx_count
    model_width = width * head_count
    span = lax.all_gather(attended, "ctx", axis=0, tiled=True)
    mine_cols = lax.dynamic_slice_in_dim(span, owner * sub, sub, 1)
    full_doc = lax.all_gather(span, "head", axis=1, tiled=True)
    slice_width = model_width // doc_count
    split_cols = full_doc.reshape(tok_rows * ctx_count, doc_count, slice_width)
    column_set = lax.all_to_all(split_cols, "doc", split_axis=1, concat_axis=0, tiled=True).reshape(
        doc_count * tok_rows * ctx_count, slice_width)
    product = lax.dot_general(
        lax.all_gather(mine_cols, "doc", axis=0, tiled=True), column_set, contract,
        preferred_element_type=jnp.float32)
    return (attended[None], product)


def solution(mesh):
    placed = (
        P("doc", "ctx", "head"),
        P("doc", "ctx", "head"),
        P("doc", "ctx", "head"),
        P("doc", None, None),
    )
    return jax.shard_map(
        per_device,
        mesh=mesh,
        in_specs=placed,
        out_specs=(P("doc", "ctx", "head"), P(("head", "ctx"), "doc")),
        check_vma=False,
    )
```
